32 devices in a mesh: rows: 16 (over z, x, core), cols: 2 (over y).
Axes of the slice: x: 2, y: 2, z: 4, core: 2. Of those that a mesh axis runs over, the one named last changes fastest.
Arguments:
- image: float32 [1024, 16384], P('rows', 'cols'), may hold values from -6 to 6
- cloud_mask: int32 [1024, 16384], P('rows', 'cols'), may hold values 0 or 1
- tile_weight: int32 [128, 128], P('rows', 'cols'), may hold values from 1 to 8
- owner: int32 [128], replicated, may hold values from 0 to 15, as said below
Outputs:
- solution: float32 [1024, 16384], P('rows', 'cols')
- objective: float32 [3], replicated
The draws below stay inside these ranges and needn't reach their ends.
Inputs may be any that keep to these rules, and one draw needn't show every extreme that they name: `owner`: every index of rows owns exactly 8 blocks, and the 8 blocks b*8 to b*8 + 7 have 8 different owners for every b.
All inputs are finite; a program needn't handle non-finite values. No bound on the sum of `cloud_mask` on one device may be relied on, other than what follows from the above.
Results may differ from the reference program's by a relative error of at most 0.0001.
Values sent between devices are 32-bit elements; how exact they have to be, the bound alone decides.
A program may use at most 64 MiB of HBM per device.

```python
import jax
import jax.numpy as jnp

BR = 8
BPD = 8
W = 16384
TW = 128
ITERS = 3
NBLK = 128
H = 1024
N_ROWS = 16


def draw_owner(key, part):
    folded = jax.random.fold_in(key, 11)
    shuffled = jax.random.permutation(jax.random.fold_in(folded, 1), N_ROWS).astype(jnp.int32)
    ranks = jnp.argsort(shuffled).astype(jnp.int32)
    values = jnp.arange(N_ROWS, dtype=jnp.int32)
    special = ((values == 1) | (values == N_ROWS // 2)).astype(jnp.int32)
    scores = ranks - 2 * N_ROWS * special
    offsets = jnp.argsort(scores).astype(jnp.int32)[:BPD]
    subkeys = jax.random.split(jax.random.fold_in(folded, 2), N_ROWS)
    orders = jax.vmap(lambda sub_key: jax.random.permutation(sub_key, BPD))(subkeys)
    source = jnp.arange(N_ROWS, dtype=jnp.int32)[:, None]
    owners = (source + offsets[orders]) % N_ROWS
    return owners.reshape(-1).astype(jnp.int32)


def set_ends(values, rng, smallest, largest):
    place = [jax.random.randint(jax.random.fold_in(rng, axis), (), 0, length) for axis, length in enumerate(values.shape)]
    longest = values.shape.index(max(values.shape))
    neighbour = place[:longest] + [(place[longest] + 1) % values.shape[longest]] + place[longest + 1:]
    return values.at[tuple(place)].set(smallest).at[tuple(neighbour)].set(largest)


def block_scale(key, extent, pieces, smallest, largest):
    gain = 1.0
    for axis_at, blocks in pieces:
        draws = jax.random.uniform(jax.random.fold_in(jax.random.fold_in(key, 6), axis_at), (blocks,), jnp.float32, smallest / len(pieces), largest / len(pieces))
        gain = gain * jnp.repeat(jnp.exp(draws), extent[axis_at] // blocks).reshape((-1,) + (1,) * (len(extent) - 1 - axis_at))
    return gain


def noise(own_key, dims, deviation, limit, cuts=(), kind=jnp.bfloat16):
    result = deviation * jax.random.normal(own_key, dims, jnp.float32)
    if cuts:
        result = result * block_scale(own_key, dims, cuts, -0.22, 0.18)
    return jnp.clip(result, -limit, limit).astype(kind)


def setup_inputs(seed: int = 0) -> dict:
    key_of = jax.random.split(jax.random.key(seed), 5)
    return {
        "image": noise(key_of[0], (H, W), 1.0, 6.0, ((0, 16), (1, 2)), jnp.float32),
        "cloud_mask": set_ends((jax.random.randint(key_of[1], (H, W), 0, 3) < 1).astype(jnp.int32), jax.random.fold_in(key_of[1], 1), 0, 1),
        "tile_weight": set_ends(jax.random.randint(key_of[2], (NBLK, W // TW), 1, 9), jax.random.fold_in(key_of[2], 1), 1, 8).astype(jnp.int32),
        "owner": draw_owner(jax.random.fold_in(key_of[4], 71), 0),
    }


fidelity_scale = 0.25
tau_step = 0.35
sigma_step = 0.35
tv_weight = 0.3

def forward_rows(field):
    return jnp.concatenate([field[1:] - field[:-1], jnp.zeros_like(field[:1])], axis=0)

def forward_cols(field):
    return jnp.concatenate([field[:, 1:] - field[:, :-1], jnp.zeros_like(field[:, :1])], axis=1)

def divergence(dual_rows, dual_cols):
    above = jnp.concatenate([jnp.zeros_like(dual_rows[:1]), dual_rows[:-1]], axis=0)
    leftward = jnp.concatenate([jnp.zeros_like(dual_cols[:, :1]), dual_cols[:, :-1]], axis=1)
    return dual_rows - above + (dual_cols - leftward)

def reference(image, cloud_mask, tile_weight, owner):
    height, width = image.shape
    total_blocks = owner.shape[0]
    tile_count = tile_weight.shape[1]
    per_tile = jnp.broadcast_to(tile_weight.astype(jnp.float32)[:, None, :, None], (total_blocks, BR, tile_count, TW)).reshape(height, width)
    fidelity = fidelity_scale * per_tile * (1 - cloud_mask).astype(jnp.float32)
    primal = image
    extrap = image
    dual_rows = jnp.zeros_like(image)
    dual_cols = jnp.zeros_like(image)
    objective_list = []
    for step in range(ITERS):
        grad_r = forward_rows(extrap)
        grad_c = forward_cols(extrap)
        trial_rows = dual_rows + sigma_step * grad_r
        trial_cols = dual_cols + sigma_step * grad_c
        shrink = jnp.maximum(1.0, jnp.sqrt(trial_rows * trial_rows + trial_cols * trial_cols) / tv_weight)
        dual_rows = trial_rows / shrink
        dual_cols = trial_cols / shrink
        updated = (primal + tau_step * divergence(dual_rows, dual_cols) + tau_step * fidelity * image) / (1.0 + tau_step * fidelity)
        misfit = updated - image
        total = jnp.sum(0.5 * fidelity * misfit * misfit) + tv_weight * jnp.sum(jnp.sqrt(grad_r * grad_r + grad_c * grad_c))
        objective_list.append(total / (height * width))
        extrap = 2.0 * updated - primal
        primal = updated
    order = jnp.argsort(owner, stable=True)
    solution = primal.reshape(total_blocks, BR, width)[order].reshape(height, width)
    return (solution, jnp.stack(objective_list).astype(jnp.float32))
```

```python
import functools

import jax
import jax.numpy as jnp
from jax import lax
from jax.experimental import pallas as pl
from jax.experimental.pallas import tpu as pltpu
from jax.sharding import PartitionSpec as P

MESH = pl.DeviceIdType.MESH
BR = 8
TW = 128
ITERS = 3
TINY = 1.2e-38

fidelity_scale = 0.25
tau_step = 0.35
sigma_step = 0.35
tv_weight = 0.3


def kernel(
    n_rows,
    n_cols,
    pixel_total,
    weight_ref,
    pick_ref,
    sender_ref,
    image_ref,
    mask_ref,
    out_ref,
    obj_ref,
    img,
    fid,
    gain,
    prim,
    extr,
    du_r,
    du_c,
    done,
    outbox,
    inbox,
    part,
    part_in,
    total,
    total_in,
    load_sem,
    halo_send,
    halo_recv,
    a2a_send,
    a2a_recv,
    part_send,
    part_recv,
    total_send,
    total_recv,
):
    rows_here, width = image_ref.shape
    blocks = rows_here // BR
    tiles = width // TW
    ext_blocks = blocks + 2
    ext_rows = rows_here + 2 * BR
    ext_tiles = tiles + 2
    me = lax.axis_index("rows")
    my_col = lax.axis_index("cols")
    has_up, has_down = me > 0, me < n_rows - 1
    has_left, has_right = my_col > 0, my_col < n_cols - 1

    load = pltpu.make_async_copy(
        image_ref, img.at[pl.ds(BR, rows_here), pl.ds(TW, width)], load_sem
    )
    load.start()

    barrier = pltpu.get_barrier_semaphore()

    @pl.loop(1, n_rows)
    def _(k):
        pl.semaphore_signal(
            barrier, inc=1, device_id={"rows": lax.rem(me + k, n_rows)}, device_id_type=MESH
        )

    @pl.loop(1, n_cols)
    def _(k):
        pl.semaphore_signal(
            barrier, inc=1, device_id={"cols": lax.rem(my_col + k, n_cols)}, device_id_type=MESH
        )

    zero_rows = jnp.zeros((BR, TW), jnp.float32)

    def fill_fid(b, t):
        col = pl.multiple_of(t * TW, TW)
        clear = (1 - mask_ref[b * BR : (b + 1) * BR, pl.ds(col, TW)]).astype(jnp.float32)
        weight = weight_ref[b, t].astype(jnp.float32)
        fid[(b + 1) * BR : (b + 2) * BR, pl.ds(col + TW, TW)] = fidelity_scale * weight * clear

    @pl.loop(0, tiles)
    def _(t):
        fill_fid(0, t)
        fill_fid(blocks - 1, t)

    @pl.loop(1, ext_tiles - 1)
    def _(t):
        at = pl.ds(pl.multiple_of(t * TW, TW), TW)

        @pl.when(jnp.logical_not(has_up))
        def _():
            img[0:BR, at] = zero_rows
            fid[0:BR, at] = zero_rows

        @pl.when(jnp.logical_not(has_down))
        def _():
            img[ext_rows - BR : ext_rows, at] = zero_rows
            fid[ext_rows - BR : ext_rows, at] = zero_rows

    zero_cols = jnp.zeros((ext_rows, TW), jnp.float32)

    @pl.when(jnp.logical_not(has_left))
    def _():
        img[:, 0:TW] = zero_cols
        fid[:, 0:TW] = zero_cols

    @pl.when(jnp.logical_not(has_right))
    def _():
        img[:, TW + width :] = zero_cols
        fid[:, TW + width :] = zero_cols

    pl.semaphore_wait(barrier, n_rows - 1 + n_cols - 1)

    inner = pl.ds(TW, width)

    def halo(index, src, dst, target):
        return pltpu.make_async_remote_copy(
            src_ref=src,
            dst_ref=dst,
            send_sem=halo_send.at[index],
            recv_sem=halo_recv.at[index],
            device_id=target,
            device_id_type=MESH,
        )

    up, down = {"rows": lax.rem(me + n_rows - 1, n_rows)}, {"rows": lax.rem(me + 1, n_rows)}
    left = {"cols": lax.rem(my_col + n_cols - 1, n_cols)}
    right = {"cols": lax.rem(my_col + 1, n_cols)}
    to_up_img = halo(
        0, image_ref.at[pl.ds(0, BR)], img.at[pl.ds(ext_rows - BR, BR), inner], up
    )
    to_up_fid = halo(1, fid.at[pl.ds(BR, BR), inner], fid.at[pl.ds(ext_rows - BR, BR), inner], up)
    to_down_img = halo(
        2, image_ref.at[pl.ds(rows_here - BR, BR)], img.at[pl.ds(0, BR), inner], down
    )
    to_down_fid = halo(
        3, fid.at[pl.ds(rows_here, BR), inner], fid.at[pl.ds(0, BR), inner], down
    )
    first, last = pl.ds(TW, TW), pl.ds(width, TW)
    beyond = pl.ds(TW + width, TW)
    to_left_img = halo(4, img.at[:, first], img.at[:, beyond], left)
    to_left_fid = halo(5, fid.at[:, first], fid.at[:, beyond], left)
    to_right_img = halo(6, img.at[:, last], img.at[:, pl.ds(0, TW)], right)
    to_right_fid = halo(7, fid.at[:, last], fid.at[:, pl.ds(0, TW)], right)

    @pl.when(has_up)
    def _():
        to_up_img.start()
        to_up_fid.start()

    @pl.when(has_down)
    def _():
        to_down_img.start()
        to_down_fid.start()

    @pl.loop(0, tiles)
    def _(t):
        for b in range(1, blocks - 1):
            fill_fid(b, t)

    load.wait()

    @pl.when(has_up)
    def _():
        to_up_img.wait_send()
        to_up_fid.wait_send()
        to_down_img.wait_recv()
        to_down_fid.wait_recv()

    @pl.when(has_down)
    def _():
        to_down_img.wait_send()
        to_down_fid.wait_send()
        to_up_img.wait_recv()
        to_up_fid.wait_recv()

    @pl.when(has_left)
    def _():
        to_left_img.start()
        to_left_fid.start()

    @pl.when(has_right)
    def _():
        to_right_img.start()
        to_right_fid.start()

    @pl.when(has_left)
    def _():
        to_left_img.wait_send()
        to_left_fid.wait_send()
        to_right_img.wait_recv()
        to_right_fid.wait_recv()

    @pl.when(has_right)
    def _():
        to_right_img.wait_send()
        to_right_fid.wait_send()
        to_left_img.wait_recv()
        to_left_fid.wait_recv()

    sub = lax.broadcasted_iota(jnp.int32, (BR, TW), 0)
    lane = lax.broadcasted_iota(jnp.int32, (BR, TW), 1)
    last_sub, first_sub = sub == BR - 1, sub == 0
    last_lane, first_lane = lane == TW - 1, lane == 0
    end_row = jnp.logical_and(last_sub, jnp.logical_not(has_down))
    end_col = jnp.logical_and(last_lane, jnp.logical_not(has_right))
    zero = jnp.zeros((BR, TW), jnp.float32)

    def one_pass(step):
        source = img if step == 0 else extr

        def at(ref, b, t):
            return ref[b * BR : (b + 1) * BR, pl.ds(pl.multiple_of(t * TW, TW), TW)]

        def body(t, carry):
            rolled, leftward, acc = carry
            after = lax.rem(t + 1, ext_tiles)
            col = pl.ds(pl.multiple_of(t * TW, TW), TW)
            stop_here = jnp.logical_and(end_col, t == tiles)
            blank = jnp.logical_and(jnp.logical_not(has_left), t == 0)
            fields = [at(source, b, t) for b in range(ext_blocks)]
            shifted = [pltpu.roll(e, BR - 1, 0) for e in fields]
            next_rolled, next_left = [], []
            above = None
            misfits, slopes = zero, zero
            for b in range(ext_blocks):
                e = fields[b]
                coming = pltpu.roll(at(source, b, after), TW - 1, 1)
                next_rolled.append(coming)
                below = shifted[min(b + 1, ext_blocks - 1)]
                g_r = jnp.where(last_sub, below, shifted[b]) - e
                g_c = jnp.where(last_lane, coming, rolled[b]) - e
                if b == blocks:
                    g_r = jnp.where(end_row, 0.0, g_r)
                g_c = jnp.where(stop_here, 0.0, g_c)
                q_r, q_c = sigma_step * g_r, sigma_step * g_c
                if step > 0:
                    q_r = q_r + at(du_r, b, t)
                    q_c = q_c + at(du_c, b, t)
                inv = jnp.minimum(1.0, tv_weight * lax.rsqrt(q_r * q_r + q_c * q_c))
                d_r, d_c = q_r * inv, q_c * inv
                if b == 0:
                    d_r = jnp.where(has_up, d_r, 0.0)
                d_c = jnp.where(blank, 0.0, d_c)
                if step < ITERS - 1:
                    du_r[b * BR : (b + 1) * BR, col] = d_r
                    du_c[b * BR : (b + 1) * BR, col] = d_c
                turned = pltpu.roll(d_r, 1, 0)
                over = turned if b == 0 else jnp.where(first_sub, above, turned)
                above = turned
                moved = pltpu.roll(d_c, 1, 1)
                before = jnp.where(first_lane, leftward[b], moved)
                next_left.append(moved)
                own = 0 < b <= blocks
                if step == ITERS - 1 and not own:
                    continue
                div = (d_r - over) + (d_c - before)
                observed = e if step == 0 else at(img, b, t)
                old = e if step == 0 else at(prim, b, t)
                f = at(fid, b, t)
                weight = tau_step * f
                if step == 0:
                    g = 1.0 / (1.0 + weight)
                    gain[b * BR : (b + 1) * BR, col] = g
                else:
                    g = at(gain, b, t)
                new = (old + tau_step * div + weight * observed) * g
                if step == ITERS - 1:
                    done[b - 1, :, col] = new
                else:
                    prim[b * BR : (b + 1) * BR, col] = new
                    extr[b * BR : (b + 1) * BR, col] = 2.0 * new - old
                if own:
                    gap = new - observed
                    misfits = misfits + f * gap * gap
                    g2 = g_r * g_r + g_c * g_c
                    slopes = slopes + g2 * lax.rsqrt(jnp.maximum(g2, TINY))
            inside = jnp.logical_and(t >= 1, t <= tiles)
            acc = acc + jnp.where(inside, 0.5 * misfits + tv_weight * slopes, 0.0)
            return next_rolled, next_left, acc

        start = [pltpu.roll(at(source, b, 0), TW - 1, 1) for b in range(ext_blocks)]
        _, _, acc = lax.fori_loop(0, ext_tiles, body, (start, [zero] * ext_blocks, zero))
        return jnp.sum(jnp.sum(acc, axis=1, keepdims=True), axis=0, keepdims=True)

    sums = [one_pass(step) for step in range(ITERS)]
    stacked = zero
    for step in range(ITERS):
        stacked = jnp.where(sub == step, sums[step], stacked)
    part[...] = stacked

    def part_copy(k):
        return pltpu.make_async_remote_copy(
            src_ref=part,
            dst_ref=part_in.at[me],
            send_sem=part_send.at[k],
            recv_sem=part_recv.at[me],
            device_id={"rows": lax.rem(me + k, n_rows)},
            device_id_type=MESH,
        )

    def block_copy(k):
        target = lax.rem(me + k, n_rows)
        return pltpu.make_async_remote_copy(
            src_ref=outbox.at[target],
            dst_ref=inbox.at[me],
            send_sem=a2a_send.at[k],
            recv_sem=a2a_recv.at[me],
            device_id={"rows": target},
            device_id_type=MESH,
        )

    def arrival(buffer, sem, source):
        return pltpu.make_async_copy(buffer.at[source], buffer.at[source], sem.at[source])

    @pl.loop(1, n_rows)
    def _(k):
        part_copy(k).start()

    @pl.loop(1, n_rows)
    def _(k):
        target = lax.rem(me + k, n_rows)
        outbox[target] = done[pick_ref[target]][:, TW : TW + width]
        block_copy(k).start()

    inbox[me] = done[pick_ref[me]][:, TW : TW + width]
    part_in[me] = stacked

    @pl.loop(1, n_rows)
    def _(k):
        arrival(part_in, part_recv, lax.rem(me + k, n_rows)).wait()

    total_here = lax.fori_loop(0, n_rows, lambda k, s: s + part_in[k], zero)
    total[...] = total_here
    total_in[my_col] = total_here

    def total_copy(k):
        return pltpu.make_async_remote_copy(
            src_ref=total,
            dst_ref=total_in.at[my_col],
            send_sem=total_send.at[k],
            recv_sem=total_recv.at[my_col],
            device_id={"cols": lax.rem(my_col + k, n_cols)},
            device_id_type=MESH,
        )

    @pl.loop(1, n_cols)
    def _(k):
        total_copy(k).start()

    @pl.loop(1, n_cols)
    def _(k):
        arrival(total_in, total_recv, lax.rem(my_col + k, n_cols)).wait()

    everything = lax.fori_loop(0, n_cols, lambda k, s: s + total_in[k], zero)
    obj_ref[...] = everything / pixel_total

    @pl.loop(1, n_rows)
    def _(k):
        arrival(inbox, a2a_recv, lax.rem(me + k, n_rows)).wait()

    for j in range(blocks):
        out_ref[j * BR : (j + 1) * BR, :] = inbox[sender_ref[j]]

    @pl.loop(1, n_rows)
    def _(k):
        block_copy(k).wait_send()
        part_copy(k).wait_send()

    @pl.loop(1, n_cols)
    def _(k):
        total_copy(k).wait_send()


def solution(mesh):
    n_rows, n_cols = mesh.shape["rows"], mesh.shape["cols"]

    def per_device(image, cloud_mask, tile_weight, owner):
        rows_here, width = image.shape
        blocks = rows_here // BR
        own_row = lax.axis_index("rows")
        pixel_total = float(owner.shape[0] * BR * width * n_cols)
        mine = lax.dynamic_slice(owner, (own_row * blocks,), (blocks,))
        devices = jnp.arange(n_rows, dtype=jnp.int32)
        local = jnp.arange(blocks, dtype=jnp.int32)
        pick = jnp.sum(
            jnp.where(mine[None, :] == devices[:, None], local[None, :], 0), axis=1, dtype=jnp.int32
        )
        owned = owner == own_row
        rank = jnp.cumsum(owned.astype(jnp.int32)) - 1
        home = jnp.arange(owner.shape[0], dtype=jnp.int32) // blocks
        sender = jnp.sum(
            jnp.where(owned[None, :] & (rank[None, :] == local[:, None]), home[None, :], 0),
            axis=1,
            dtype=jnp.int32,
        )
        ext = (rows_here + 2 * BR, width + 2 * TW)
        small = (BR, TW)
        vmem = pl.BlockSpec(memory_space=pltpu.VMEM)
        smem = pl.BlockSpec(memory_space=pltpu.SMEM)
        f32 = jnp.float32
        dma = pltpu.SemaphoreType.DMA
        out, obj = pl.pallas_call(
            functools.partial(kernel, n_rows, n_cols, pixel_total),
            out_shape=(
                jax.ShapeDtypeStruct((rows_here, width), f32),
                jax.ShapeDtypeStruct(small, f32),
            ),
            in_specs=[smem, smem, smem, pl.BlockSpec(memory_space=pl.ANY), vmem],
            out_specs=(vmem, vmem),
            scratch_shapes=[pltpu.VMEM(ext, f32)] * 7
            + [pltpu.VMEM((blocks, BR, width + 2 * TW), f32)]
            + [pltpu.VMEM((n_rows, BR, width), f32)] * 2
            + [
                pltpu.VMEM(small, f32),
                pltpu.VMEM((n_rows,) + small, f32),
                pltpu.VMEM(small, f32),
                pltpu.VMEM((n_cols,) + small, f32),
                dma,
                dma((8,)),
                dma((8,)),
                dma((n_rows,)),
                dma((n_rows,)),
                dma((n_rows,)),
                dma((n_rows,)),
                dma((n_cols,)),
                dma((n_cols,)),
            ],
            compiler_params=pltpu.CompilerParams(
                collective_id=0, has_side_effects=True, vmem_limit_bytes=60 * 1024 * 1024
            ),
        )(tile_weight, pick, sender, image, cloud_mask)
        return out, obj[:ITERS, 0]

    in_specs = (P("rows", "cols"), P("rows", "cols"), P("rows", "cols"), P())
    out_specs = (P("rows", "cols"), P())
    return jax.shard_map(
        per_device, mesh=mesh, in_specs=in_specs, out_specs=out_specs, check_vma=False
    )
```

```python
import functools

import jax
import jax.numpy as jnp
from jax import lax
from jax.experimental import pallas as pl
from jax.experimental.pallas import tpu as pltpu
from jax.sharding import PartitionSpec as P

MESH = pl.DeviceIdType.MESH
BR = 8
TW = 128
ITERS = 3
TINY = 1.2e-38

fidelity_scale = 0.25
tau_step = 0.35
sigma_step = 0.35
tv_weight = 0.3


def kernel(
    n_rows,
    n_cols,
    pixel_total,
    weight_ref,
    image_ref,
    mask_ref,
    out_ref,
    obj_ref,
    img,
    fid,
    gain,
    prim,
    extr,
    du_r,
    du_c,
    part,
    part_in,
    total,
    total_in,
    load_sem,
    halo_send,
    halo_recv,
    part_send,
    part_recv,
    total_send,
    total_recv,
):
    rows_here, width = image_ref.shape
    blocks = rows_here // BR
    tiles = width // TW
    ext_blocks = blocks + 2
    ext_rows = rows_here + 2 * BR
    ext_tiles = tiles + 2
    me = lax.axis_index("rows")
    my_col = lax.axis_index("cols")
    has_up, has_down = me > 0, me < n_rows - 1
    has_left, has_right = my_col > 0, my_col < n_cols - 1

    load = pltpu.make_async_copy(
        image_ref, img.at[pl.ds(BR, rows_here), pl.ds(TW, width)], load_sem
    )
    load.start()

    barrier = pltpu.get_barrier_semaphore()

    @pl.loop(1, n_rows)
    def _(k):
        pl.semaphore_signal(
            barrier, inc=1, device_id={"rows": lax.rem(me + k, n_rows)}, device_id_type=MESH
        )

    @pl.loop(1, n_cols)
    def _(k):
        pl.semaphore_signal(
            barrier, inc=1, device_id={"cols": lax.rem(my_col + k, n_cols)}, device_id_type=MESH
        )

    zero_rows = jnp.zeros((BR, TW), jnp.float32)

    def fill_fid(b, t):
        col = pl.multiple_of(t * TW, TW)
        clear = (1 - mask_ref[b * BR : (b + 1) * BR, pl.ds(col, TW)]).astype(jnp.float32)
        weight = weight_ref[b, t].astype(jnp.float32)
        fid[(b + 1) * BR : (b + 2) * BR, pl.ds(col + TW, TW)] = fidelity_scale * weight * clear

    @pl.loop(0, tiles)
    def _(t):
        fill_fid(0, t)
        fill_fid(blocks - 1, t)

    @pl.loop(1, ext_tiles - 1)
    def _(t):
        at = pl.ds(pl.multiple_of(t * TW, TW), TW)

        @pl.when(jnp.logical_not(has_up))
        def _():
            img[0:BR, at] = zero_rows
            fid[0:BR, at] = zero_rows

        @pl.when(jnp.logical_not(has_down))
        def _():
            img[ext_rows - BR : ext_rows, at] = zero_rows
            fid[ext_rows - BR : ext_rows, at] = zero_rows

    zero_cols = jnp.zeros((ext_rows, TW), jnp.float32)

    @pl.when(jnp.logical_not(has_left))
    def _():
        img[:, 0:TW] = zero_cols
        fid[:, 0:TW] = zero_cols

    @pl.when(jnp.logical_not(has_right))
    def _():
        img[:, TW + width :] = zero_cols
        fid[:, TW + width :] = zero_cols

    pl.semaphore_wait(barrier, n_rows - 1 + n_cols - 1)

    inner = pl.ds(TW, width)

    def halo(index, src, dst, target):
        return pltpu.make_async_remote_copy(
            src_ref=src,
            dst_ref=dst,
            send_sem=halo_send.at[index],
            recv_sem=halo_recv.at[index],
            device_id=target,
            device_id_type=MESH,
        )

    up, down = {"rows": lax.rem(me + n_rows - 1, n_rows)}, {"rows": lax.rem(me + 1, n_rows)}
    left = {"cols": lax.rem(my_col + n_cols - 1, n_cols)}
    right = {"cols": lax.rem(my_col + 1, n_cols)}
    to_up_img = halo(
        0, image_ref.at[pl.ds(0, BR)], img.at[pl.ds(ext_rows - BR, BR), inner], up
    )
    to_up_fid = halo(1, fid.at[pl.ds(BR, BR), inner], fid.at[pl.ds(ext_rows - BR, BR), inner], up)
    to_down_img = halo(
        2, image_ref.at[pl.ds(rows_here - BR, BR)], img.at[pl.ds(0, BR), inner], down
    )
    to_down_fid = halo(
        3, fid.at[pl.ds(rows_here, BR), inner], fid.at[pl.ds(0, BR), inner], down
    )
    first, last = pl.ds(TW, TW), pl.ds(width, TW)
    beyond = pl.ds(TW + width, TW)
    to_left_img = halo(4, img.at[:, first], img.at[:, beyond], left)
    to_left_fid = halo(5, fid.at[:, first], fid.at[:, beyond], left)
    to_right_img = halo(6, img.at[:, last], img.at[:, pl.ds(0, TW)], right)
    to_right_fid = halo(7, fid.at[:, last], fid.at[:, pl.ds(0, TW)], right)

    @pl.when(has_up)
    def _():
        to_up_img.start()
        to_up_fid.start()

    @pl.when(has_down)
    def _():
        to_down_img.start()
        to_down_fid.start()

    @pl.loop(0, tiles)
    def _(t):
        for b in range(1, blocks - 1):
            fill_fid(b, t)

    load.wait()

    @pl.when(has_up)
    def _():
        to_up_img.wait_send()
        to_up_fid.wait_send()
        to_down_img.wait_recv()
        to_down_fid.wait_recv()

    @pl.when(has_down)
    def _():
        to_down_img.wait_send()
        to_down_fid.wait_send()
        to_up_img.wait_recv()
        to_up_fid.wait_recv()

    @pl.when(has_left)
    def _():
        to_left_img.start()
        to_left_fid.start()

    @pl.when(has_right)
    def _():
        to_right_img.start()
        to_right_fid.start()

    @pl.when(has_left)
    def _():
        to_left_img.wait_send()
        to_left_fid.wait_send()
        to_right_img.wait_recv()
        to_right_fid.wait_recv()

    @pl.when(has_right)
    def _():
        to_right_img.wait_send()
        to_right_fid.wait_send()
        to_left_img.wait_recv()
        to_left_fid.wait_recv()

    sub = lax.broadcasted_iota(jnp.int32, (BR, TW), 0)
    lane = lax.broadcasted_iota(jnp.int32, (BR, TW), 1)
    last_sub, first_sub = sub == BR - 1, sub == 0
    last_lane, first_lane = lane == TW - 1, lane == 0
    end_row = jnp.logical_and(last_sub, jnp.logical_not(has_down))
    end_col = jnp.logical_and(last_lane, jnp.logical_not(has_right))
    zero = jnp.zeros((BR, TW), jnp.float32)

    def one_pass(step):
        source = img if step == 0 else extr
        stop = ext_tiles - 1 if step == ITERS - 1 else ext_tiles

        def at(ref, b, t):
            return ref[b * BR : (b + 1) * BR, pl.ds(pl.multiple_of(t * TW, TW), TW)]

        def body(t, carry):
            rolled, leftward, acc = carry
            after = lax.rem(t + 1, ext_tiles)
            inner_col = pl.ds(pl.multiple_of(lax.rem(t + tiles - 1, tiles) * TW, TW), TW)
            col = pl.ds(pl.multiple_of(t * TW, TW), TW)
            stop_here = jnp.logical_and(end_col, t == tiles)
            blank = jnp.logical_and(jnp.logical_not(has_left), t == 0)
            fields = [at(source, b, t) for b in range(ext_blocks)]
            shifted = [pltpu.roll(e, BR - 1, 0) for e in fields]
            next_rolled, next_left = [], []
            above = None
            misfits, slopes = zero, zero
            for b in range(ext_blocks):
                e = fields[b]
                coming = pltpu.roll(at(source, b, after), TW - 1, 1)
                next_rolled.append(coming)
                below = shifted[min(b + 1, ext_blocks - 1)]
                g_r = jnp.where(last_sub, below, shifted[b]) - e
                g_c = jnp.where(last_lane, coming, rolled[b]) - e
                if b == blocks:
                    g_r = jnp.where(end_row, 0.0, g_r)
                g_c = jnp.where(stop_here, 0.0, g_c)
                q_r, q_c = sigma_step * g_r, sigma_step * g_c
                if step > 0:
                    q_r = q_r + at(du_r, b, t)
                    q_c = q_c + at(du_c, b, t)
                inv = jnp.minimum(1.0, tv_weight * lax.rsqrt(q_r * q_r + q_c * q_c))
                d_r, d_c = q_r * inv, q_c * inv
                if b == 0:
                    d_r = jnp.where(has_up, d_r, 0.0)
                d_c = jnp.where(blank, 0.0, d_c)
                if step < ITERS - 1:
                    du_r[b * BR : (b + 1) * BR, col] = d_r
                    du_c[b * BR : (b + 1) * BR, col] = d_c
                turned = pltpu.roll(d_r, 1, 0)
                over = turned if b == 0 else jnp.where(first_sub, above, turned)
                above = turned
                moved = pltpu.roll(d_c, 1, 1)
                before = jnp.where(first_lane, leftward[b], moved)
                next_left.append(moved)
                own = 0 < b <= blocks
                if step == ITERS - 1 and not own:
                    continue
                div = (d_r - over) + (d_c - before)
                observed = e if step == 0 else at(img, b, t)
                old = e if step == 0 else at(prim, b, t)
                f = at(fid, b, t)
                weight = tau_step * f
                if step == 0:
                    g = 1.0 / (1.0 + weight)
                    gain[b * BR : (b + 1) * BR, col] = g
                else:
                    g = at(gain, b, t)
                new = (old + tau_step * div + weight * observed) * g
                if step == ITERS - 1:
                    out_ref[(b - 1) * BR : b * BR, inner_col] = new
                else:
                    prim[b * BR : (b + 1) * BR, col] = new
                    extr[b * BR : (b + 1) * BR, col] = 2.0 * new - old
                if own:
                    gap = new - observed
                    misfits = misfits + f * gap * gap
                    g2 = g_r * g_r + g_c * g_c
                    slopes = slopes + g2 * lax.rsqrt(jnp.maximum(g2, TINY))
            inside = jnp.logical_and(t >= 1, t <= tiles)
            acc = acc + jnp.where(inside, 0.5 * misfits + tv_weight * slopes, 0.0)
            return next_rolled, next_left, acc

        start = [pltpu.roll(at(source, b, 0), TW - 1, 1) for b in range(ext_blocks)]
        _, _, acc = lax.fori_loop(0, stop, body, (start, [zero] * ext_blocks, zero))
        return jnp.sum(jnp.sum(acc, axis=1, keepdims=True), axis=0, keepdims=True)

    sums = [one_pass(step) for step in range(ITERS)]
    stacked = zero
    for step in range(ITERS):
        stacked = jnp.where(sub == step, sums[step], stacked)
    part[...] = stacked

    def part_copy(k):
        return pltpu.make_async_remote_copy(
            src_ref=part,
            dst_ref=part_in.at[me],
            send_sem=part_send.at[k],
            recv_sem=part_recv.at[me],
            device_id={"rows": lax.rem(me + k, n_rows)},
            device_id_type=MESH,
        )

    def arrival(buffer, sem, source):
        return pltpu.make_async_copy(buffer.at[source], buffer.at[source], sem.at[source])

    @pl.loop(1, n_rows)
    def _(k):
        part_copy(k).start()

    part_in[me] = stacked

    @pl.loop(1, n_rows)
    def _(k):
        arrival(part_in, part_recv, lax.rem(me + k, n_rows)).wait()

    total_here = lax.fori_loop(0, n_rows, lambda k, s: s + part_in[k], zero)
    total[...] = total_here
    total_in[my_col] = total_here

    def total_copy(k):
        return pltpu.make_async_remote_copy(
            src_ref=total,
            dst_ref=total_in.at[my_col],
            send_sem=total_send.at[k],
            recv_sem=total_recv.at[my_col],
            device_id={"cols": lax.rem(my_col + k, n_cols)},
            device_id_type=MESH,
        )

    @pl.loop(1, n_cols)
    def _(k):
        total_copy(k).start()

    @pl.loop(1, n_cols)
    def _(k):
        arrival(total_in, total_recv, lax.rem(my_col + k, n_cols)).wait()

    everything = lax.fori_loop(0, n_cols, lambda k, s: s + total_in[k], zero)
    obj_ref[...] = everything / pixel_total

    @pl.loop(1, n_rows)
    def _(k):
        part_copy(k).wait_send()

    @pl.loop(1, n_cols)
    def _(k):
        total_copy(k).wait_send()


def rounds_of(n_rows):
    half = n_rows // 2
    pairs = [(k, n_rows - k) for k in range(1, half)]
    groups = [(half,) + pairs[0]] if pairs else [(half,)]
    return groups + pairs[1:]


def hand_over(primal, owner, pick, sender, n_rows):
    rows_here, width = primal.shape
    blocks = rows_here // BR
    me = lax.axis_index("rows")
    home = jnp.arange(owner.shape[0], dtype=jnp.int32) // blocks
    distance = lax.rem(owner - home + n_rows, n_rows)
    used = jnp.any(distance[None, :] == jnp.arange(n_rows, dtype=jnp.int32)[:, None], axis=1)
    used = used.astype(jnp.int32)

    def outgoing(k):
        at = pick[lax.rem(me + k, n_rows)] * BR
        return lax.dynamic_slice(primal, (at, 0), (BR, width))

    def placed(result, block, k):
        source = lax.rem(me + n_rows - k, n_rows)
        here = sender == source
        at = jnp.argmax(here).astype(jnp.int32) * BR
        held = lax.dynamic_slice(result, (at, 0), (BR, width))
        return lax.dynamic_update_slice(result, jnp.where(jnp.any(here), block, held), (at, 0))

    def run(chosen, result):
        arrived = [
            lax.ppermute(outgoing(k), "rows", [(i, (i + k) % n_rows) for i in range(n_rows)])
            for k in chosen
        ]
        for k, block in zip(chosen, arrived):
            result = placed(result, block, k)
        return result

    result = placed(jnp.zeros_like(primal), outgoing(0), 0)
    for group in rounds_of(n_rows):
        code = sum(used[k] << i for i, k in enumerate(group))
        subsets = [
            tuple(k for i, k in enumerate(group) if (c >> i) & 1) for c in range(1 << len(group))
        ]
        result = lax.switch(code, [functools.partial(run, chosen) for chosen in subsets], result)
    return result


def solution(mesh):
    n_rows, n_cols = mesh.shape["rows"], mesh.shape["cols"]

    def per_device(image, cloud_mask, tile_weight, owner):
        rows_here, width = image.shape
        blocks = rows_here // BR
        own_row = lax.axis_index("rows")
        pixel_total = float(owner.shape[0] * BR * width * n_cols)
        mine = lax.dynamic_slice(owner, (own_row * blocks,), (blocks,))
        devices = jnp.arange(n_rows, dtype=jnp.int32)
        local = jnp.arange(blocks, dtype=jnp.int32)
        pick = jnp.sum(
            jnp.where(mine[None, :] == devices[:, None], local[None, :], 0), axis=1, dtype=jnp.int32
        )
        owned = owner == own_row
        rank = jnp.cumsum(owned.astype(jnp.int32)) - 1
        home = jnp.arange(owner.shape[0], dtype=jnp.int32) // blocks
        sender = jnp.sum(
            jnp.where(owned[None, :] & (rank[None, :] == local[:, None]), home[None, :], 0),
            axis=1,
            dtype=jnp.int32,
        )
        ext = (rows_here + 2 * BR, width + 2 * TW)
        small = (BR, TW)
        vmem = pl.BlockSpec(memory_space=pltpu.VMEM)
        smem = pl.BlockSpec(memory_space=pltpu.SMEM)
        f32 = jnp.float32
        dma = pltpu.SemaphoreType.DMA
        out, obj = pl.pallas_call(
            functools.partial(kernel, n_rows, n_cols, pixel_total),
            out_shape=(
                jax.ShapeDtypeStruct((rows_here, width), f32),
                jax.ShapeDtypeStruct(small, f32),
            ),
            in_specs=[smem, pl.BlockSpec(memory_space=pl.ANY), vmem],
            out_specs=(vmem, vmem),
            scratch_shapes=[pltpu.VMEM(ext, f32)] * 7
            + [
                pltpu.VMEM(small, f32),
                pltpu.VMEM((n_rows,) + small, f32),
                pltpu.VMEM(small, f32),
                pltpu.VMEM((n_cols,) + small, f32),
                dma,
                dma((8,)),
                dma((8,)),
                dma((n_rows,)),
                dma((n_rows,)),
                dma((n_cols,)),
                dma((n_cols,)),
            ],
            compiler_params=pltpu.CompilerParams(
                collective_id=0, has_side_effects=True, vmem_limit_bytes=60 * 1024 * 1024
            ),
        )(tile_weight, image, cloud_mask)
        moved = hand_over(out, owner, pick, sender, n_rows)
        return moved, obj[:ITERS, 0]

    in_specs = (P("rows", "cols"), P("rows", "cols"), P("rows", "cols"), P())
    out_specs = (P("rows", "cols"), P())
    return jax.shard_map(
        per_device, mesh=mesh, in_specs=in_specs, out_specs=out_specs, check_vma=False
    )
```

```python
import functools

import jax
import jax.numpy as jnp
from jax import lax
from jax.experimental import pallas as pl
from jax.experimental.pallas import tpu as pltpu
from jax.sharding import PartitionSpec as P

MESH = pl.DeviceIdType.MESH
BR = 8
TW = 128
ITERS = 3
TINY = 1.2e-38

fidelity_scale = 0.25
tau_step = 0.35
sigma_step = 0.35
tv_weight = 0.3


def kernel(
    n_rows,
    n_cols,
    pixel_total,
    weight_ref,
    pick_ref,
    sender_ref,
    image_ref,
    mask_ref,
    out_ref,
    obj_ref,
    img,
    fid,
    gain,
    prim,
    extr,
    du_r,
    du_c,
    done,
    outbox,
    inbox,
    part,
    part_in,
    total,
    total_in,
    load_sem,
    halo_send,
    halo_recv,
    a2a_send,
    a2a_recv,
    part_send,
    part_recv,
    total_send,
    total_recv,
):
    rows_here, width = image_ref.shape
    blocks = rows_here // BR
    tiles = width // TW
    ext_blocks = blocks + 2
    ext_rows = rows_here + 2 * BR
    ext_tiles = tiles + 2
    me = lax.axis_index("rows")
    my_col = lax.axis_index("cols")
    has_up, has_down = me > 0, me < n_rows - 1
    has_left, has_right = my_col > 0, my_col < n_cols - 1

    load = pltpu.make_async_copy(
        image_ref, img.at[pl.ds(BR, rows_here), pl.ds(TW, width)], load_sem
    )
    load.start()

    barrier = pltpu.get_barrier_semaphore()

    @pl.loop(1, n_rows)
    def _(k):
        pl.semaphore_signal(
            barrier, inc=1, device_id={"rows": lax.rem(me + k, n_rows)}, device_id_type=MESH
        )

    @pl.loop(1, n_cols)
    def _(k):
        pl.semaphore_signal(
            barrier, inc=1, device_id={"cols": lax.rem(my_col + k, n_cols)}, device_id_type=MESH
        )

    zero_rows = jnp.zeros((BR, TW), jnp.float32)

    def fill_fid(b, t):
        col = pl.multiple_of(t * TW, TW)
        clear = (1 - mask_ref[b * BR : (b + 1) * BR, pl.ds(col, TW)]).astype(jnp.float32)
        weight = weight_ref[b, t].astype(jnp.float32)
        fid[(b + 1) * BR : (b + 2) * BR, pl.ds(col + TW, TW)] = fidelity_scale * weight * clear

    @pl.loop(0, tiles)
    def _(t):
        fill_fid(0, t)
        fill_fid(blocks - 1, t)

    @pl.loop(1, ext_tiles - 1)
    def _(t):
        at = pl.ds(pl.multiple_of(t * TW, TW), TW)

        @pl.when(jnp.logical_not(has_up))
        def _():
            img[0:BR, at] = zero_rows
            fid[0:BR, at] = zero_rows

        @pl.when(jnp.logical_not(has_down))
        def _():
            img[ext_rows - BR : ext_rows, at] = zero_rows
            fid[ext_rows - BR : ext_rows, at] = zero_rows

    zero_cols = jnp.zeros((ext_rows, TW), jnp.float32)

    @pl.when(jnp.logical_not(has_left))
    def _():
        img[:, 0:TW] = zero_cols
        fid[:, 0:TW] = zero_cols

    @pl.when(jnp.logical_not(has_right))
    def _():
        img[:, TW + width :] = zero_cols
        fid[:, TW + width :] = zero_cols

    pl.semaphore_wait(barrier, n_rows - 1 + n_cols - 1)

    inner = pl.ds(TW, width)

    def halo(index, src, dst, target):
        return pltpu.make_async_remote_copy(
            src_ref=src,
            dst_ref=dst,
            send_sem=halo_send.at[index],
            recv_sem=halo_recv.at[index],
            device_id=target,
            device_id_type=MESH,
        )

    up, down = {"rows": lax.rem(me + n_rows - 1, n_rows)}, {"rows": lax.rem(me + 1, n_rows)}
    left = {"cols": lax.rem(my_col + n_cols - 1, n_cols)}
    right = {"cols": lax.rem(my_col + 1, n_cols)}
    to_up_img = halo(
        0, image_ref.at[pl.ds(0, BR)], img.at[pl.ds(ext_rows - BR, BR), inner], up
    )
    to_up_fid = halo(1, fid.at[pl.ds(BR, BR), inner], fid.at[pl.ds(ext_rows - BR, BR), inner], up)
    to_down_img = halo(
        2, image_ref.at[pl.ds(rows_here - BR, BR)], img.at[pl.ds(0, BR), inner], down
    )
    to_down_fid = halo(
        3, fid.at[pl.ds(rows_here, BR), inner], fid.at[pl.ds(0, BR), inner], down
    )
    first, last = pl.ds(TW, TW), pl.ds(width, TW)
    beyond = pl.ds(TW + width, TW)
    to_left_img = halo(4, img.at[:, first], img.at[:, beyond], left)
    to_left_fid = halo(5, fid.at[:, first], fid.at[:, beyond], left)
    to_right_img = halo(6, img.at[:, last], img.at[:, pl.ds(0, TW)], right)
    to_right_fid = halo(7, fid.at[:, last], fid.at[:, pl.ds(0, TW)], right)

    @pl.when(has_up)
    def _():
        to_up_img.start()
        to_up_fid.start()

    @pl.when(has_down)
    def _():
        to_down_img.start()
        to_down_fid.start()

    @pl.loop(0, tiles)
    def _(t):
        for b in range(1, blocks - 1):
            fill_fid(b, t)

    load.wait()

    @pl.when(has_up)
    def _():
        to_up_img.wait_send()
        to_up_fid.wait_send()
        to_down_img.wait_recv()
        to_down_fid.wait_recv()

    @pl.when(has_down)
    def _():
        to_down_img.wait_send()
        to_down_fid.wait_send()
        to_up_img.wait_recv()
        to_up_fid.wait_recv()

    @pl.when(has_left)
    def _():
        to_left_img.start()
        to_left_fid.start()

    @pl.when(has_right)
    def _():
        to_right_img.start()
        to_right_fid.start()

    @pl.when(has_left)
    def _():
        to_left_img.wait_send()
        to_left_fid.wait_send()
        to_right_img.wait_recv()
        to_right_fid.wait_recv()

    @pl.when(has_right)
    def _():
        to_right_img.wait_send()
        to_right_fid.wait_send()
        to_left_img.wait_recv()
        to_left_fid.wait_recv()

    sub = lax.broadcasted_iota(jnp.int32, (BR, TW), 0)
    lane = lax.broadcasted_iota(jnp.int32, (BR, TW), 1)
    last_sub, first_sub = sub == BR - 1, sub == 0
    last_lane, first_lane = lane == TW - 1, lane == 0
    end_row = jnp.logical_and(last_sub, jnp.logical_not(has_down))
    end_col = jnp.logical_and(last_lane, jnp.logical_not(has_right))
    zero = jnp.zeros((BR, TW), jnp.float32)

    def one_pass(step):
        source = img if step == 0 else extr

        def at(ref, b, t):
            return ref[b * BR : (b + 1) * BR, pl.ds(pl.multiple_of(t * TW, TW), TW)]

        def body(t, carry):
            rolled, leftward, acc = carry
            after = lax.rem(t + 1, ext_tiles)
            col = pl.ds(pl.multiple_of(t * TW, TW), TW)
            stop_here = jnp.logical_and(end_col, t == tiles)
            blank = jnp.logical_and(jnp.logical_not(has_left), t == 0)
            fields = [at(source, b, t) for b in range(ext_blocks)]
            shifted = [pltpu.roll(e, BR - 1, 0) for e in fields]
            coming = [pltpu.roll(at(source, b, after), TW - 1, 1) for b in range(ext_blocks)]
            slopes_r, slopes_c, duals_r, duals_c = [], [], [], []
            for b in range(ext_blocks):
                e = fields[b]
                below = shifted[min(b + 1, ext_blocks - 1)]
                g_r = jnp.where(last_sub, below, shifted[b]) - e
                g_c = jnp.where(last_lane, coming[b], rolled[b]) - e
                if b == blocks:
                    g_r = jnp.where(end_row, 0.0, g_r)
                g_c = jnp.where(stop_here, 0.0, g_c)
                q_r, q_c = sigma_step * g_r, sigma_step * g_c
                if step > 0:
                    q_r = q_r + at(du_r, b, t)
                    q_c = q_c + at(du_c, b, t)
                inv = jnp.minimum(1.0, tv_weight * lax.rsqrt(q_r * q_r + q_c * q_c))
                d_r, d_c = q_r * inv, q_c * inv
                if b == 0:
                    d_r = jnp.where(has_up, d_r, 0.0)
                d_c = jnp.where(blank, 0.0, d_c)
                slopes_r.append(g_r)
                slopes_c.append(g_c)
                duals_r.append(d_r)
                duals_c.append(d_c)
            turned = [pltpu.roll(d, 1, 0) for d in duals_r]
            moved = [pltpu.roll(d, 1, 1) for d in duals_c]
            slopes = zero
            for b in range(1, blocks + 1):
                g2 = slopes_r[b] * slopes_r[b] + slopes_c[b] * slopes_c[b]
                slopes = slopes + g2 * lax.rsqrt(jnp.maximum(g2, TINY))
            misfits = zero
            writes = []
            for b in range(ext_blocks):
                own = 0 < b <= blocks
                if step == ITERS - 1 and not own:
                    continue
                rows = slice(b * BR, (b + 1) * BR)
                over = turned[b] if b == 0 else jnp.where(first_sub, turned[b - 1], turned[b])
                before = jnp.where(first_lane, leftward[b], moved[b])
                div = (duals_r[b] - over) + (duals_c[b] - before)
                observed = fields[b] if step == 0 else at(img, b, t)
                old = fields[b] if step == 0 else at(prim, b, t)
                f = at(fid, b, t)
                weight = tau_step * f
                if step == 0:
                    g = 1.0 / (1.0 + weight)
                    writes.append((gain, rows, g))
                else:
                    g = at(gain, b, t)
                new = (old + tau_step * div + weight * observed) * g
                if step == ITERS - 1:
                    writes.append((done, b - 1, new))
                else:
                    writes.append((prim, rows, new))
                    writes.append((extr, rows, 2.0 * new - old))
                    writes.append((du_r, rows, duals_r[b]))
                    writes.append((du_c, rows, duals_c[b]))
                if own:
                    gap = new - observed
                    misfits = misfits + f * gap * gap
            for ref, rows, value in writes:
                if ref is done:
                    ref[rows, :, col] = value
                else:
                    ref[rows, col] = value
            next_rolled, next_left = coming, moved
            inside = jnp.logical_and(t >= 1, t <= tiles)
            acc = acc + jnp.where(inside, 0.5 * misfits + tv_weight * slopes, 0.0)
            return next_rolled, next_left, acc

        start = [pltpu.roll(at(source, b, 0), TW - 1, 1) for b in range(ext_blocks)]
        _, _, acc = lax.fori_loop(0, ext_tiles, body, (start, [zero] * ext_blocks, zero))
        return jnp.sum(jnp.sum(acc, axis=1, keepdims=True), axis=0, keepdims=True)

    sums = [one_pass(step) for step in range(ITERS)]
    stacked = zero
    for step in range(ITERS):
        stacked = jnp.where(sub == step, sums[step], stacked)
    part[...] = stacked

    def part_copy(k):
        return pltpu.make_async_remote_copy(
            src_ref=part,
            dst_ref=part_in.at[me],
            send_sem=part_send.at[k],
            recv_sem=part_recv.at[me],
            device_id={"rows": lax.rem(me + k, n_rows)},
            device_id_type=MESH,
        )

    def block_copy(k):
        target = lax.rem(me + k, n_rows)
        return pltpu.make_async_remote_copy(
            src_ref=outbox.at[target],
            dst_ref=inbox.at[me],
            send_sem=a2a_send.at[k],
            recv_sem=a2a_recv.at[me],
            device_id={"rows": target},
            device_id_type=MESH,
        )

    def arrival(buffer, sem, source):
        return pltpu.make_async_copy(buffer.at[source], buffer.at[source], sem.at[source])

    @pl.loop(1, n_rows)
    def _(k):
        part_copy(k).start()

    @pl.loop(1, n_rows)
    def _(k):
        target = lax.rem(me + k, n_rows)
        outbox[target] = done[pick_ref[target]][:, TW : TW + width]
        block_copy(k).start()

    inbox[me] = done[pick_ref[me]][:, TW : TW + width]
    part_in[me] = stacked

    @pl.loop(1, n_rows)
    def _(k):
        arrival(part_in, part_recv, lax.rem(me + k, n_rows)).wait()

    total_here = lax.fori_loop(0, n_rows, lambda k, s: s + part_in[k], zero)
    total[...] = total_here
    total_in[my_col] = total_here

    def total_copy(k):
        return pltpu.make_async_remote_copy(
            src_ref=total,
            dst_ref=total_in.at[my_col],
            send_sem=total_send.at[k],
            recv_sem=total_recv.at[my_col],
            device_id={"cols": lax.rem(my_col + k, n_cols)},
            device_id_type=MESH,
        )

    @pl.loop(1, n_cols)
    def _(k):
        total_copy(k).start()

    @pl.loop(1, n_cols)
    def _(k):
        arrival(total_in, total_recv, lax.rem(my_col + k, n_cols)).wait()

    everything = lax.fori_loop(0, n_cols, lambda k, s: s + total_in[k], zero)
    obj_ref[...] = everything / pixel_total

    @pl.loop(1, n_rows)
    def _(k):
        arrival(inbox, a2a_recv, lax.rem(me + k, n_rows)).wait()

    for j in range(blocks):
        out_ref[j * BR : (j + 1) * BR, :] = inbox[sender_ref[j]]

    @pl.loop(1, n_rows)
    def _(k):
        block_copy(k).wait_send()
        part_copy(k).wait_send()

    @pl.loop(1, n_cols)
    def _(k):
        total_copy(k).wait_send()


def solution(mesh):
    n_rows, n_cols = mesh.shape["rows"], mesh.shape["cols"]

    def per_device(image, cloud_mask, tile_weight, owner):
        rows_here, width = image.shape
        blocks = rows_here // BR
        own_row = lax.axis_index("rows")
        pixel_total = float(owner.shape[0] * BR * width * n_cols)
        mine = lax.dynamic_slice(owner, (own_row * blocks,), (blocks,))
        devices = jnp.arange(n_rows, dtype=jnp.int32)
        local = jnp.arange(blocks, dtype=jnp.int32)
        pick = jnp.sum(
            jnp.where(mine[None, :] == devices[:, None], local[None, :], 0), axis=1, dtype=jnp.int32
        )
        owned = owner == own_row
        rank = jnp.cumsum(owned.astype(jnp.int32)) - 1
        home = jnp.arange(owner.shape[0], dtype=jnp.int32) // blocks
        sender = jnp.sum(
            jnp.where(owned[None, :] & (rank[None, :] == local[:, None]), home[None, :], 0),
            axis=1,
            dtype=jnp.int32,
        )
        ext = (rows_here + 2 * BR, width + 2 * TW)
        small = (BR, TW)
        vmem = pl.BlockSpec(memory_space=pltpu.VMEM)
        smem = pl.BlockSpec(memory_space=pltpu.SMEM)
        f32 = jnp.float32
        dma = pltpu.SemaphoreType.DMA
        out, obj = pl.pallas_call(
            functools.partial(kernel, n_rows, n_cols, pixel_total),
            out_shape=(
                jax.ShapeDtypeStruct((rows_here, width), f32),
                jax.ShapeDtypeStruct(small, f32),
            ),
            in_specs=[smem, smem, smem, pl.BlockSpec(memory_space=pl.ANY), vmem],
            out_specs=(vmem, vmem),
            scratch_shapes=[pltpu.VMEM(ext, f32)] * 7
            + [pltpu.VMEM((blocks, BR, width + 2 * TW), f32)]
            + [pltpu.VMEM((n_rows, BR, width), f32)] * 2
            + [
                pltpu.VMEM(small, f32),
                pltpu.VMEM((n_rows,) + small, f32),
                pltpu.VMEM(small, f32),
                pltpu.VMEM((n_cols,) + small, f32),
                dma,
                dma((8,)),
                dma((8,)),
                dma((n_rows,)),
                dma((n_rows,)),
                dma((n_rows,)),
                dma((n_rows,)),
                dma((n_cols,)),
                dma((n_cols,)),
            ],
            compiler_params=pltpu.CompilerParams(
                collective_id=0, has_side_effects=True, vmem_limit_bytes=60 * 1024 * 1024
            ),
        )(tile_weight, pick, sender, image, cloud_mask)
        return out, obj[:ITERS, 0]

    in_specs = (P("rows", "cols"), P("rows", "cols"), P("rows", "cols"), P())
    out_specs = (P("rows", "cols"), P())
    return jax.shard_map(
        per_device, mesh=mesh, in_specs=in_specs, out_specs=out_specs, check_vma=False
    )
```
